16 devices in a mesh: ens: 2 (over y, z), feat: 8 (over x, core).
Axes of the slice: x: 4, y: 2, z: 1, core: 2. Of those that a mesh axis runs over, the one named last changes fastest.
The devices are a block of a 4x4x8 slice.
Arguments:
- particles: float32 [4, 512, 16384], P('ens', None, 'feat'), parts along dimension 0
- target_mean: float32 [4, 16384], P('ens', 'feat'), parts along dimension 0
- precision: float32 [32768], P(('ens', 'feat')), parts along dimension 0
- low_factor: bfloat16 [32768, 64], P(('ens', 'feat')), parts along dimension 0
Outputs:
- output: float32 [4, 512, 16384], P('ens', None, 'feat'), parts along dimension 0
There are 2 independent parts. The reference program is written for one: setup_inputs(seed, part) draws one part's arguments, and reference() takes and returns one part's arrays. A program takes and returns all parts, laid end to end along the dimension named above; each array names one.
All inputs are finite; a program needn't handle non-finite values.
Results may differ from the reference program's by a relative error of at most 0.001.
Values are sent between devices in bfloat16 or wider.
A program may use at most 768 MiB of HBM per device.

```python
import jax
import jax.numpy as jnp
from jax import lax

PARTICLES = 512
FEATURES = 16384
LOW_RANK = 64
NUM_STEPS = 3


def setup_inputs(seed: int = 0, part: int = 0) -> dict:
    base_key = jax.random.fold_in(jax.random.key(seed), part)
    key_list = jax.random.split(base_key, 7)
    prec_scale = 2.0 / FEATURES
    factor_scale = prec_scale ** 0.5 / FEATURES ** 0.5
    low_raw = factor_scale * jax.random.normal(key_list[0], (FEATURES, LOW_RANK), jnp.float32)
    precision = prec_scale * jax.random.uniform(key_list[1], (FEATURES,), jnp.float32, 0.5, 1.5)
    target_mean = jax.random.normal(key_list[2], (2, FEATURES), jnp.float32)
    center = 0.7 * jax.random.normal(key_list[3], (2, FEATURES), jnp.float32)
    coef_vec = jax.random.normal(key_list[4], (2, LOW_RANK), jnp.float32)
    aligned = jnp.dot(coef_vec, low_raw.T) * (0.7 / (factor_scale * LOW_RANK ** 0.5))
    spread = jax.random.uniform(key_list[5], (2, PARTICLES, 1), jnp.float32, 0.5, 1.5)
    noise_mat = jax.random.normal(key_list[6], (2, PARTICLES, FEATURES), jnp.float32)
    particles = (target_mean + center + aligned)[:, None, :] + spread * noise_mat
    return {"particles": particles, "target_mean": target_mean, "precision": precision, "low_factor": low_raw.astype(jnp.bfloat16)}


def svgd_step(theta, target_mean, precision, low_factor):
    bandwidth = 2.0 * FEATURES
    step_size = 0.25 * FEATURES
    low_wide = low_factor.astype(jnp.float32)
    centered = theta - target_mean[:, None, :]
    project = jnp.einsum("end,dr->enr", centered.astype(jnp.bfloat16).astype(jnp.float32), low_wide)
    theta_wide = theta.astype(jnp.bfloat16).astype(jnp.float32)
    gram_mat = jnp.einsum("end,emd->enm", theta_wide, theta_wide)
    gram_diag = jnp.diagonal(gram_mat, axis1=1, axis2=2)
    sq_dist = jnp.maximum(gram_diag[:, :, None] + gram_diag[:, None, :] - 2.0 * gram_mat, 0.0)
    kernel = jnp.exp(-sq_dist / bandwidth)
    low_term = jnp.einsum("enr,dr->end", project.astype(jnp.bfloat16).astype(jnp.float32), low_wide)
    grad_log = -(centered * precision + low_term)
    mixed = (grad_log - (2.0 / bandwidth) * theta).astype(jnp.bfloat16).astype(jnp.float32)
    drive = jnp.einsum("enm,emd->end", kernel.astype(jnp.bfloat16).astype(jnp.float32), mixed)
    row_sum = jnp.sum(kernel, axis=2, keepdims=True)
    return theta + step_size * ((drive + (2.0 / bandwidth) * row_sum * theta) / PARTICLES)


def reference(particles, target_mean, precision, low_factor):
    def scan_body(theta, unused):
        return svgd_step(theta, target_mean, precision, low_factor), None
    final_theta, unused_out = lax.scan(scan_body, particles, None, length=NUM_STEPS)
    return final_theta
```

```python
import functools

import jax
import jax.numpy as jnp
from jax import lax
from jax.experimental import pallas as pl
from jax.experimental.pallas import tpu as pltpu
from jax.sharding import PartitionSpec as P

NUM_STEPS = 3
MESH = pl.DeviceIdType.MESH
NT = (((1,), (1,)), ((), ()))
CHUNKS = 4
TILE = 512
VMEM_LIMIT = 60 * 1024 * 1024


def dot_nt(a, b):
    return lax.dot_general(a, b, NT, preferred_element_type=jnp.float32)


def exchange_kernel(cores, chips, part_hbm, mean_ref, prec_ref, low_ref,
                    theta_hbm, kern_out, proj_out, sums_out,
                    theta, theta_bf, drift, factor2, kern, proj, sums, proj_part, gram,
                    gbuf, dbuf, gsib, dsib, acc, dacc, gpeer, dpeer, kbuf, sbuf,
                    load_sem, store_sem, s1_send, s1_recv, s2_send, s2_recv, s3_send, s3_recv, s4_send, s4_recv):
    num_ens, num_part, loc_feat = theta.shape
    half = num_part // 2
    core_rows = half // cores
    piece = core_rows // chips
    bandwidth = 2.0 * loc_feat * cores * chips
    step_size = 0.25 * loc_feat * cores * chips

    me = lax.axis_index("feat")
    core = lax.rem(me, cores)
    chip = lax.div(me, cores)
    sibling = chip * cores + (1 - core)
    my_core_row = pl.multiple_of(core * core_rows, core_rows)
    sib_core_row = pl.multiple_of((1 - core) * core_rows, core_rows)
    my_piece_row = pl.multiple_of(my_core_row + chip * piece, piece)

    def chip_at(offset):
        return lax.rem(chip + offset, chips)

    def peer(offset):
        return chip_at(offset) * cores + core

    def remote(src, dst, send, recv, dev):
        return pltpu.make_async_remote_copy(src_ref=src, dst_ref=dst, send_sem=send, recv_sem=recv,
                                            device_id={"feat": dev}, device_id_type=MESH)

    rows = num_part // CHUNKS
    loads = {}
    for e in range(num_ens):
        for c in range(CHUNKS):
            loads[e, c] = pltpu.make_async_copy(part_hbm.at[e, pl.ds(c * rows, rows)],
                                                theta.at[e, pl.ds(c * rows, rows)], load_sem.at[e * CHUNKS + c])
            loads[e, c].start()

    barrier = pltpu.get_barrier_semaphore()
    for offset in range(1, cores * chips):
        pl.semaphore_signal(barrier, inc=1, device_id={"feat": lax.rem(me + offset, cores * chips)}, device_id_type=MESH)

    factor2[...] = jnp.concatenate([low_ref[...], low_ref[...]], axis=1)
    rank2 = factor2.shape[1]
    rank = rank2 // 2
    lane_low = lax.broadcasted_iota(jnp.int32, (half, rank2), 1) < rank
    row_id = lax.broadcasted_iota(jnp.int32, (half, half), 0)
    col_id = lax.broadcasted_iota(jnp.int32, (half, half), 1)

    def first_rows(e):
        for c in range(CHUNKS):
            loads[e, c].wait()
            sl = pl.ds(c * rows, rows)
            th = theta[e, sl, :]
            theta_bf[e, sl, :] = th.astype(jnp.bfloat16)
            xb = (th - mean_ref[e:e + 1, :]).astype(jnp.bfloat16)
            proj_part[e, sl, :] = jnp.dot(xb, factor2[...], preferred_element_type=jnp.float32)

    def gram_and_pack(e):
        gram[...] = dot_nt(theta_bf[e], theta_bf[e])
        g00 = gram[0:half, 0:half]
        g11 = gram[half:, half:]
        gbuf[e, :, 0:half] = jnp.where(col_id >= row_id, g00, g11)
        gbuf[e, :, half:2 * half] = gram[0:half, half:]
        gbuf[e, :, 2 * half:] = jnp.where(lane_low, proj_part[e, 0:half, :], proj_part[e, half:, :])
        d0 = jnp.sum(jnp.where(col_id == row_id, g00, 0.0), axis=0, keepdims=True)
        d1 = jnp.sum(jnp.where(col_id == row_id, g11, 0.0), axis=0, keepdims=True)
        dbuf[e] = jnp.concatenate([d0, d1, jnp.zeros((6, half), jnp.float32)], axis=0)

    def s1(e):
        return (remote(gbuf.at[e, pl.ds(sib_core_row, core_rows)], gsib.at[e], s1_send.at[2 * e], s1_recv.at[2 * e], sibling),
                remote(dbuf.at[e], dsib.at[e], s1_send.at[2 * e + 1], s1_recv.at[2 * e + 1], sibling))

    def s2(e, k):
        i = 2 * (e * chips + k)
        return (remote(acc.at[e, pl.ds(pl.multiple_of(chip_at(k) * piece, piece), piece)], gpeer.at[e, k - 1],
                       s2_send.at[i], s2_recv.at[i], peer(k)),
                remote(dacc.at[e], dpeer.at[e, k - 1], s2_send.at[i + 1], s2_recv.at[i + 1], peer(k)))

    def s3(e, k):
        i = 2 * (e * chips + k)
        mine = pl.ds(my_piece_row, piece)
        return (remote(kbuf.at[e, mine], kbuf.at[e, mine], s3_send.at[i], s3_recv.at[i], peer(k)),
                remote(sbuf.at[e, core * chips + chip], sbuf.at[e, core * chips + chip],
                       s3_send.at[i + 1], s3_recv.at[i + 1], peer(k)))

    def s3_in(e, k):
        i = 2 * (e * chips + k)
        src = chip_at(chips - k)
        rws = pl.ds(pl.multiple_of(my_core_row + src * piece, piece), piece)
        return (remote(kbuf.at[e, rws], kbuf.at[e, rws], s3_send.at[i], s3_recv.at[i], peer(chips - k)),
                remote(sbuf.at[e, core * chips + src], sbuf.at[e, core * chips + src],
                       s3_send.at[i + 1], s3_recv.at[i + 1], peer(chips - k)))

    def s4(e, k, owner_core):
        i = 2 * (e * chips + k)
        src = chip_at(chips - k)
        rws = pl.ds(pl.multiple_of(owner_core * core_rows + src * piece, piece), piece)
        return (remote(kbuf.at[e, rws], kbuf.at[e, rws], s4_send.at[i], s4_recv.at[i], sibling),
                remote(sbuf.at[e, owner_core * chips + src], sbuf.at[e, owner_core * chips + src],
                       s4_send.at[i + 1], s4_recv.at[i + 1], sibling))

    pending = {}

    def send(key, copies):
        for c in copies:
            c.start()
        pending.setdefault(key, []).extend(copies)

    def drain(key):
        for c in pending.pop(key, []):
            c.wait_send()

    def start_s1(e):
        send(("s1", e), s1(e))

    def mid_s1(e):
        for c in s1(e):
            c.wait_recv()
        drain(("s2", e))
        acc[e] = gbuf[e, pl.ds(my_core_row, core_rows), :] + gsib[e]
        dacc[e] = dbuf[e] + dsib[e]
        drain(("s1", e))
        for k in range(1, chips):
            send(("s2", e), s2(e, k))

    def mid_s2(e):
        for k in range(1, chips):
            for c in s2(e, k):
                c.wait_recv()
        own = acc[e, pl.ds(pl.multiple_of(chip * piece, piece), piece), :]
        dg = dacc[e]
        for k in range(1, chips):
            own = own + gpeer[e, k - 1]
            dg = dg + dpeer[e, k - 1]
        l0 = dg[0:1, :]
        l1 = dg[1:2, :]
        col = lax.broadcasted_iota(jnp.int32, (piece, half), 1)
        row = lax.broadcasted_iota(jnp.int32, (piece, half), 0) + my_piece_row
        on = col == row
        up = col >= row
        c0 = jnp.sum(jnp.where(on, l0, 0.0), axis=1, keepdims=True)
        c1 = jnp.sum(jnp.where(on, l1, 0.0), axis=1, keepdims=True)
        dist_t = jnp.maximum(jnp.where(up, c0 + l0, c1 + l1) - 2.0 * own[:, 0:half], 0.0)
        dist_o = jnp.maximum((c0 + l1) - 2.0 * own[:, half:2 * half], 0.0)
        k_t = jnp.where(on, 1.0, jnp.exp(-dist_t / bandwidth))
        k_o = jnp.exp(-dist_o / bandwidth)
        mine = pl.ds(my_piece_row, piece)
        kbuf[e, mine, 0:half] = k_t.astype(jnp.bfloat16)
        kbuf[e, mine, half:2 * half] = k_o.astype(jnp.bfloat16)
        kbuf[e, mine, 2 * half:] = own[:, 2 * half:].astype(jnp.bfloat16)
        low = col < row
        row0 = jnp.sum(jnp.where(up, k_t, 0.0) + k_o, axis=1, keepdims=True)
        row1 = jnp.sum(jnp.where(low, k_t, 0.0), axis=1, keepdims=True) + 1.0
        s0 = jnp.sum(jnp.where(col > row, k_t, 0.0) + jnp.where(on, row0, 0.0), axis=0, keepdims=True)
        s1_ = jnp.sum(jnp.where(low, k_t, 0.0) + k_o + jnp.where(on, row1, 0.0), axis=0, keepdims=True)
        sbuf[e, core * chips + chip] = jnp.concatenate([s0, s1_, jnp.zeros((6, half), jnp.float32)], axis=0)
        for k in range(1, chips):
            send(("s3", e), s3(e, k))
        send(("s4", e), s4(e, 0, core))

    def mid_s3(e):
        for k in sorted(range(1, chips), key=lambda k: min(k, chips - k)):
            for c in s3_in(e, k):
                c.wait_recv()
            send(("s4", e), s4(e, k, core))

    def unpack(e, kern_ref, proj_ref, sums_ref):
        for k in range(chips):
            for c in s4(e, k, 1 - core):
                c.wait_recv()
        drain(("s3", e))
        drain(("s4", e))
        t = kbuf[e, :, 0:half].astype(jnp.float32)
        tt = t.T
        kern_ref[0:half, 0:half] = jnp.where(col_id >= row_id, t, tt).astype(jnp.bfloat16)
        kern_ref[half:, half:] = jnp.where(col_id <= row_id, t, tt).astype(jnp.bfloat16)
        ko = kbuf[e, :, half:2 * half]
        kern_ref[0:half, half:] = ko
        kern_ref[half:, 0:half] = ko.astype(jnp.float32).T.astype(jnp.bfloat16)
        pj = kbuf[e, :, 2 * half:].astype(jnp.float32)
        proj_ref[0:half, :] = jnp.where(lane_low, pj, 0.0).astype(jnp.bfloat16)
        proj_ref[half:, :] = jnp.where(lane_low, 0.0, pj).astype(jnp.bfloat16)
        tot = sbuf[e, 0]
        for o in range(1, cores * chips):
            tot = tot + sbuf[e, o]
        tot = (2.0 / bandwidth) * tot
        for q in range(num_part // 128):
            r = q * 128 // half
            lo = q * 128 % half
            line = tot[r:r + 1, lo:lo + 128]
            sums_ref[pl.ds(q * 128, 128), :] = jnp.broadcast_to(line, (128, 128)).T

    def update(e):
        for t in range(loc_feat // TILE):
            sl = pl.ds(t * TILE, TILE)
            th = theta[e, :, sl]
            low = dot_nt(proj[...], factor2[sl, :])
            yn = (th - mean_ref[e:e + 1, sl]) * prec_ref[0:1, sl] + low + (2.0 / bandwidth) * th
            drift[...] = yn.astype(jnp.bfloat16)
            drive = jnp.dot(kern[...], drift[...], preferred_element_type=jnp.float32)
            srow = jnp.concatenate([sums[...]] * (TILE // 128), axis=1)
            new = th + step_size * ((srow * th - drive) / num_part)
            theta[e, :, sl] = new
            theta_bf[e, :, sl] = new.astype(jnp.bfloat16)
            xb = (new - mean_ref[e:e + 1, sl]).astype(jnp.bfloat16)
            part = jnp.dot(xb, factor2[sl, :], preferred_element_type=jnp.float32)
            if t == 0:
                proj_part[e] = part
            else:
                proj_part[e] += part

    first_rows(0)
    gram_and_pack(0)
    pl.semaphore_wait(barrier, cores * chips - 1)
    start_s1(0)
    first_rows(1)
    mid_s1(0)
    gram_and_pack(1)
    start_s1(1)
    stores = []
    for step in range(NUM_STEPS):
        mid_s1(1)
        mid_s2(0)
        mid_s2(1)
        mid_s3(0)
        if step < NUM_STEPS - 1:
            unpack(0, kern, proj, sums)
            update(0)
            mid_s3(1)
            gram_and_pack(0)
            start_s1(0)
            unpack(1, kern, proj, sums)
            update(1)
            mid_s1(0)
            gram_and_pack(1)
            start_s1(1)
            if step == NUM_STEPS - 2:
                for e in range(num_ens):
                    st = pltpu.make_async_copy(theta.at[e], theta_hbm.at[e], store_sem.at[e])
                    st.start()
                    stores.append(st)
        else:
            unpack(0, kern_out.at[0], proj_out.at[0], sums_out.at[0])
            mid_s3(1)
            unpack(1, kern_out.at[1], proj_out.at[1], sums_out.at[1])
    for st in stores:
        st.wait()
    for key in list(pending):
        drain(key)


def final_kernel(bandwidth, step_size, num_part, th_ref, kern_ref, proj_ref, sums_ref, mean_ref, prec_ref, low_ref, out_ref):
    th = th_ref[0]
    width = th.shape[1]
    low_t = low_ref[...]
    low = dot_nt(proj_ref[0], jnp.concatenate([low_t, low_t], axis=1))
    yn = (th - mean_ref[0]) * prec_ref[...] + low + (2.0 / bandwidth) * th
    drive = jnp.dot(kern_ref[0], yn.astype(jnp.bfloat16), preferred_element_type=jnp.float32)
    srow = jnp.concatenate([sums_ref[0]] * (width // 128), axis=1)
    out_ref[0] = th + step_size * ((srow * th - drive) / num_part)


def solution(mesh):
    feat_count = mesh.shape["feat"]
    cores = 2
    chips = feat_count // cores
    data_spec = P("ens", None, "feat")
    mean_spec = P("ens", "feat")
    prec_spec = P(("ens", "feat"))
    factor_spec = P(("ens", "feat"), None)

    def local_steps(particles, target_mean, precision, low_factor):
        num_ens, num_part, loc_feat = particles.shape
        rank = low_factor.shape[1]
        half = num_part // 2
        core_rows = half // cores
        piece = core_rows // chips
        width = 2 * half + 2 * rank
        bandwidth = 2.0 * loc_feat * feat_count
        step_size = 0.25 * loc_feat * feat_count
        prec_row = precision.reshape(1, loc_feat)
        f32, bf16 = jnp.float32, jnp.bfloat16
        vmem = pl.BlockSpec(memory_space=pltpu.VMEM)
        anyspace = pl.BlockSpec(memory_space=pl.ANY)
        dma = pltpu.SemaphoreType.DMA
        nsem = 2 * num_ens * chips
        theta, kern, proj, sums = pl.pallas_call(
            functools.partial(exchange_kernel, cores, chips),
            out_shape=(
                jax.ShapeDtypeStruct((num_ens, num_part, loc_feat), f32),
                jax.ShapeDtypeStruct((num_ens, num_part, num_part), bf16),
                jax.ShapeDtypeStruct((num_ens, num_part, 2 * rank), bf16),
                jax.ShapeDtypeStruct((num_ens, num_part, 128), f32),
            ),
            in_specs=[anyspace, vmem, vmem, vmem],
            out_specs=(anyspace, vmem, vmem, vmem),
            scratch_shapes=[
                pltpu.VMEM((num_ens, num_part, loc_feat), f32),
                pltpu.VMEM((num_ens, num_part, loc_feat), bf16),
                pltpu.VMEM((num_part, TILE), bf16),
                pltpu.VMEM((loc_feat, 2 * rank), bf16),
                pltpu.VMEM((num_part, num_part), bf16),
                pltpu.VMEM((num_part, 2 * rank), bf16),
                pltpu.VMEM((num_part, 128), f32),
                pltpu.VMEM((num_ens, num_part, 2 * rank), f32),
                pltpu.VMEM((num_part, num_part), f32),
                pltpu.VMEM((num_ens, half, width), f32),
                pltpu.VMEM((num_ens, 8, half), f32),
                pltpu.VMEM((num_ens, core_rows, width), f32),
                pltpu.VMEM((num_ens, 8, half), f32),
                pltpu.VMEM((num_ens, core_rows, width), f32),
                pltpu.VMEM((num_ens, 8, half), f32),
                pltpu.VMEM((num_ens, chips - 1, piece, width), f32),
                pltpu.VMEM((num_ens, chips - 1, 8, half), f32),
                pltpu.VMEM((num_ens, half, width), bf16),
                pltpu.VMEM((num_ens, feat_count, 8, half), f32),
                dma((num_ens * CHUNKS,)),
                dma((num_ens,)),
                dma((2 * num_ens,)), dma((2 * num_ens,)),
                dma((nsem,)), dma((nsem,)),
                dma((nsem,)), dma((nsem,)),
                dma((nsem,)), dma((nsem,)),
            ],
            compiler_params=pltpu.CompilerParams(
                collective_id=0, has_side_effects=True, vmem_limit_bytes=VMEM_LIMIT),
            name="exchange",
        )(particles, target_mean, prec_row, low_factor)
        tiles = loc_feat // TILE
        return pl.pallas_call(
            functools.partial(final_kernel, bandwidth, step_size, num_part),
            out_shape=jax.ShapeDtypeStruct((num_ens, num_part, loc_feat), f32),
            grid=(num_ens, tiles),
            in_specs=[
                pl.BlockSpec((1, num_part, TILE), lambda e, t: (e, 0, t)),
                pl.BlockSpec((1, num_part, num_part), lambda e, t: (e, 0, 0)),
                pl.BlockSpec((1, num_part, 2 * rank), lambda e, t: (e, 0, 0)),
                pl.BlockSpec((1, num_part, 128), lambda e, t: (e, 0, 0)),
                pl.BlockSpec((1, 1, TILE), lambda e, t: (e, 0, t)),
                pl.BlockSpec((1, TILE), lambda e, t: (0, t)),
                pl.BlockSpec((TILE, rank), lambda e, t: (t, 0)),
            ],
            out_specs=pl.BlockSpec((1, num_part, TILE), lambda e, t: (e, 0, t)),
            name="final_update",
        )(theta, kern, proj, sums, target_mean[:, None, :], prec_row, low_factor)

    return jax.shard_map(local_steps, mesh=mesh, in_specs=(data_spec, mean_spec, prec_spec, factor_spec),
                         out_specs=data_spec, check_vma=False)
```

```python
import functools

import jax
import jax.numpy as jnp
from jax import lax
from jax.experimental import pallas as pl
from jax.experimental.pallas import tpu as pltpu
from jax.sharding import PartitionSpec as P

NUM_STEPS = 3
MESH = pl.DeviceIdType.MESH
NT = (((1,), (1,)), ((), ()))
CHUNKS = 4
TILE = 512
VMEM_LIMIT = 40 * 1024 * 1024
FINAL_LIMIT = 20 * 1024 * 1024


def dot_nt(a, b):
    return lax.dot_general(a, b, NT, preferred_element_type=jnp.float32)


def advance(th, kern, proj, sums, mean, prec, fact, bandwidth, step_size, num_part):
    low = jnp.dot(proj[...], fact, preferred_element_type=jnp.float32)
    yn = (th - mean) * prec + low + (2.0 / bandwidth) * th
    drive = jnp.dot(kern[...], yn.astype(jnp.bfloat16), preferred_element_type=jnp.float32)
    srow = jnp.concatenate([sums[...]] * (th.shape[1] // 128), axis=1)
    return th + step_size * ((srow * th - drive) / num_part)


def exchange_kernel(cores, chips, part_hbm, mean_ref, prec_ref, low_ref,
                    theta, kern_out, proj_out, sums_out,
                    theta_bf, factor2, kern, proj, sums, proj_part, gram,
                    gbuf, dbuf, gsib, dsib, acc, dacc, gpeer, dpeer, kbuf, sbuf,
                    load_sem, s1_send, s1_recv, s2_send, s2_recv, s3_send, s3_recv, s4_send, s4_recv):
    num_ens, num_part, loc_feat = theta.shape
    half = num_part // 2
    core_rows = half // cores
    piece = core_rows // chips
    bandwidth = 2.0 * loc_feat * cores * chips
    step_size = 0.25 * loc_feat * cores * chips

    me = lax.axis_index("feat")
    core = lax.rem(me, cores)
    chip = lax.div(me, cores)
    sibling = chip * cores + (1 - core)
    my_core_row = pl.multiple_of(core * core_rows, core_rows)
    sib_core_row = pl.multiple_of((1 - core) * core_rows, core_rows)
    my_piece_row = pl.multiple_of(my_core_row + chip * piece, piece)

    def chip_at(offset):
        return lax.rem(chip + offset, chips)

    def peer(offset):
        return chip_at(offset) * cores + core

    def remote(src, dst, send, recv, dev):
        return pltpu.make_async_remote_copy(src_ref=src, dst_ref=dst, send_sem=send, recv_sem=recv,
                                            device_id={"feat": dev}, device_id_type=MESH)

    rows = num_part // CHUNKS
    loads = {}
    for e in range(num_ens):
        for c in range(CHUNKS):
            loads[e, c] = pltpu.make_async_copy(part_hbm.at[e, pl.ds(c * rows, rows)],
                                                theta.at[e, pl.ds(c * rows, rows)], load_sem.at[e * CHUNKS + c])
            loads[e, c].start()

    barrier = pltpu.get_barrier_semaphore()
    for offset in range(1, cores * chips):
        pl.semaphore_signal(barrier, inc=1, device_id={"feat": lax.rem(me + offset, cores * chips)}, device_id_type=MESH)

    factor2[...] = jnp.concatenate([low_ref[...], low_ref[...]], axis=0)
    rank2 = factor2.shape[0]
    rank = rank2 // 2
    lane_low = lax.broadcasted_iota(jnp.int32, (half, rank2), 1) < rank
    row_id = lax.broadcasted_iota(jnp.int32, (half, half), 0)
    col_id = lax.broadcasted_iota(jnp.int32, (half, half), 1)

    def first_rows(e):
        for c in range(CHUNKS):
            loads[e, c].wait()
            sl = pl.ds(c * rows, rows)
            th = theta[e, sl, :]
            theta_bf[e, sl, :] = th.astype(jnp.bfloat16)
            xb = (th - mean_ref[e:e + 1, :]).astype(jnp.bfloat16)
            proj_part[e, sl, :] = dot_nt(xb, factor2[...])

    def gram_and_pack(e):
        gram[...] = dot_nt(theta_bf[e], theta_bf[e])
        g00 = gram[0:half, 0:half]
        g11 = gram[half:, half:]
        gbuf[e, :, 0:half] = jnp.where(col_id >= row_id, g00, g11)
        gbuf[e, :, half:2 * half] = gram[0:half, half:]
        gbuf[e, :, 2 * half:] = jnp.where(lane_low, proj_part[e, 0:half, :], proj_part[e, half:, :])
        d0 = jnp.sum(jnp.where(col_id == row_id, g00, 0.0), axis=0, keepdims=True)
        d1 = jnp.sum(jnp.where(col_id == row_id, g11, 0.0), axis=0, keepdims=True)
        dbuf[e] = jnp.concatenate([d0, d1, jnp.zeros((6, half), jnp.float32)], axis=0)

    def s1(e):
        return (remote(gbuf.at[e, pl.ds(sib_core_row, core_rows)], gsib.at[e], s1_send.at[2 * e], s1_recv.at[2 * e], sibling),
                remote(dbuf.at[e], dsib.at[e], s1_send.at[2 * e + 1], s1_recv.at[2 * e + 1], sibling))

    def s2(e, k):
        i = 2 * (e * chips + k)
        return (remote(acc.at[e, pl.ds(pl.multiple_of(chip_at(k) * piece, piece), piece)], gpeer.at[e, k - 1],
                       s2_send.at[i], s2_recv.at[i], peer(k)),
                remote(dacc.at[e], dpeer.at[e, k - 1], s2_send.at[i + 1], s2_recv.at[i + 1], peer(k)))

    def s3(e, k):
        i = 2 * (e * chips + k)
        mine = pl.ds(my_piece_row, piece)
        return (remote(kbuf.at[e, mine], kbuf.at[e, mine], s3_send.at[i], s3_recv.at[i], peer(k)),
                remote(sbuf.at[e, core * chips + chip], sbuf.at[e, core * chips + chip],
                       s3_send.at[i + 1], s3_recv.at[i + 1], peer(k)))

    def s3_in(e, k):
        i = 2 * (e * chips + k)
        src = chip_at(chips - k)
        rws = pl.ds(pl.multiple_of(my_core_row + src * piece, piece), piece)
        return (remote(kbuf.at[e, rws], kbuf.at[e, rws], s3_send.at[i], s3_recv.at[i], peer(chips - k)),
                remote(sbuf.at[e, core * chips + src], sbuf.at[e, core * chips + src],
                       s3_send.at[i + 1], s3_recv.at[i + 1], peer(chips - k)))

    def s4(e, k, owner_core):
        i = 2 * (e * chips + k)
        src = chip_at(chips - k)
        rws = pl.ds(pl.multiple_of(owner_core * core_rows + src * piece, piece), piece)
        return (remote(kbuf.at[e, rws], kbuf.at[e, rws], s4_send.at[i], s4_recv.at[i], sibling),
                remote(sbuf.at[e, owner_core * chips + src], sbuf.at[e, owner_core * chips + src],
                       s4_send.at[i + 1], s4_recv.at[i + 1], sibling))

    pending = {}

    def send(key, copies):
        for c in copies:
            c.start()
        pending.setdefault(key, []).extend(copies)

    def drain(key):
        for c in pending.pop(key, []):
            c.wait_send()

    def start_s1(e):
        send(("s1", e), s1(e))

    def mid_s1(e):
        for c in s1(e):
            c.wait_recv()
        drain(("s2", e))
        acc[e] = gbuf[e, pl.ds(my_core_row, core_rows), :] + gsib[e]
        dacc[e] = dbuf[e] + dsib[e]
        drain(("s1", e))
        for k in range(1, chips):
            send(("s2", e), s2(e, k))

    def mid_s2(e):
        for k in range(1, chips):
            for c in s2(e, k):
                c.wait_recv()
        own = acc[e, pl.ds(pl.multiple_of(chip * piece, piece), piece), :]
        dg = dacc[e]
        for k in range(1, chips):
            own = own + gpeer[e, k - 1]
            dg = dg + dpeer[e, k - 1]
        l0 = dg[0:1, :]
        l1 = dg[1:2, :]
        col = lax.broadcasted_iota(jnp.int32, (piece, half), 1)
        row = lax.broadcasted_iota(jnp.int32, (piece, half), 0) + my_piece_row
        on = col == row
        up = col >= row
        c0 = jnp.sum(jnp.where(on, l0, 0.0), axis=1, keepdims=True)
        c1 = jnp.sum(jnp.where(on, l1, 0.0), axis=1, keepdims=True)
        dist_t = jnp.maximum(jnp.where(up, c0 + l0, c1 + l1) - 2.0 * own[:, 0:half], 0.0)
        dist_o = jnp.maximum((c0 + l1) - 2.0 * own[:, half:2 * half], 0.0)
        k_t = jnp.where(on, 1.0, jnp.exp(-dist_t / bandwidth))
        k_o = jnp.exp(-dist_o / bandwidth)
        mine = pl.ds(my_piece_row, piece)
        kbuf[e, mine, 0:half] = k_t.astype(jnp.bfloat16)
        kbuf[e, mine, half:2 * half] = k_o.astype(jnp.bfloat16)
        kbuf[e, mine, 2 * half:] = own[:, 2 * half:].astype(jnp.bfloat16)
        low = col < row
        row0 = jnp.sum(jnp.where(up, k_t, 0.0) + k_o, axis=1, keepdims=True)
        row1 = jnp.sum(jnp.where(low, k_t, 0.0), axis=1, keepdims=True) + 1.0
        s0 = jnp.sum(jnp.where(col > row, k_t, 0.0) + jnp.where(on, row0, 0.0), axis=0, keepdims=True)
        s1_ = jnp.sum(jnp.where(low, k_t, 0.0) + k_o + jnp.where(on, row1, 0.0), axis=0, keepdims=True)
        sbuf[e, core * chips + chip] = jnp.concatenate([s0, s1_, jnp.zeros((6, half), jnp.float32)], axis=0)
        for k in range(1, chips):
            send(("s3", e), s3(e, k))
        send(("s4", e), s4(e, 0, core))

    def mid_s3(e):
        for k in sorted(range(1, chips), key=lambda k: min(k, chips - k)):
            for c in s3_in(e, k):
                c.wait_recv()
            send(("s4", e), s4(e, k, core))

    def unpack(e, kern_ref, proj_ref, sums_ref):
        for k in range(chips):
            for c in s4(e, k, 1 - core):
                c.wait_recv()
        drain(("s3", e))
        drain(("s4", e))
        t = kbuf[e, :, 0:half].astype(jnp.float32)
        tt = t.T
        kern_ref[0:half, 0:half] = jnp.where(col_id >= row_id, t, tt).astype(jnp.bfloat16)
        kern_ref[half:, half:] = jnp.where(col_id <= row_id, t, tt).astype(jnp.bfloat16)
        ko = kbuf[e, :, half:2 * half]
        kern_ref[0:half, half:] = ko
        kern_ref[half:, 0:half] = ko.astype(jnp.float32).T.astype(jnp.bfloat16)
        pj = kbuf[e, :, 2 * half:].astype(jnp.float32)
        proj_ref[0:half, :] = jnp.where(lane_low, pj, 0.0).astype(jnp.bfloat16)
        proj_ref[half:, :] = jnp.where(lane_low, 0.0, pj).astype(jnp.bfloat16)
        tot = sbuf[e, 0]
        for o in range(1, cores * chips):
            tot = tot + sbuf[e, o]
        tot = (2.0 / bandwidth) * tot
        for q in range(num_part // 128):
            r = q * 128 // half
            lo = q * 128 % half
            line = tot[r:r + 1, lo:lo + 128]
            sums_ref[pl.ds(q * 128, 128), :] = jnp.broadcast_to(line, (128, 128)).T

    def update(e, last):
        for t in range(loc_feat // TILE):
            sl = pl.ds(t * TILE, TILE)
            new = advance(theta[e, :, sl], kern, proj, sums, mean_ref[e:e + 1, sl], prec_ref[0:1, sl],
                          factor2[:, sl], bandwidth, step_size, num_part)
            theta[e, :, sl] = new
            if last:
                continue
            theta_bf[e, :, sl] = new.astype(jnp.bfloat16)
            xb = (new - mean_ref[e:e + 1, sl]).astype(jnp.bfloat16)
            part = dot_nt(xb, factor2[:, sl])
            if t == 0:
                proj_part[e] = part
            else:
                proj_part[e] += part

    first_rows(0)
    gram_and_pack(0)
    pl.semaphore_wait(barrier, cores * chips - 1)
    start_s1(0)
    first_rows(1)
    mid_s1(0)
    gram_and_pack(1)
    start_s1(1)
    for step in range(NUM_STEPS):
        last = step == NUM_STEPS - 1
        mid_s1(1)
        mid_s2(0)
        mid_s2(1)
        mid_s3(0)
        unpack(0, kern, proj, sums)
        if last:
            mid_s3(1)
            update(0, True)
            unpack(1, kern_out, proj_out, sums_out)
        else:
            update(0, False)
            mid_s3(1)
            gram_and_pack(0)
            start_s1(0)
            unpack(1, kern, proj, sums)
            update(1, False)
            mid_s1(0)
            gram_and_pack(1)
            start_s1(1)
    for key in list(pending):
        drain(key)


def final_kernel(bandwidth, step_size, theta, kern, proj, sums, mean_ref, prec_ref, low_ref, out_hbm, done, store_sem):
    num_ens, num_part, loc_feat = theta.shape
    stores = []
    for e in range(num_ens - 1):
        stores.append(pltpu.make_async_copy(theta.at[e], out_hbm.at[e], store_sem.at[e]))
        stores[-1].start()
    e = num_ens - 1
    for t in range(loc_feat // TILE):
        sl = pl.ds(t * TILE, TILE)
        low_t = low_ref[:, sl]
        done[t] = advance(theta[e, :, sl], kern, proj, sums, mean_ref[e:e + 1, sl], prec_ref[0:1, sl],
                          jnp.concatenate([low_t, low_t], axis=0), bandwidth, step_size, num_part)
        stores.append(pltpu.make_async_copy(done.at[t], out_hbm.at[e, :, sl], store_sem.at[e + t]))
        stores[-1].start()
    for st in stores:
        st.wait()


def solution(mesh):
    feat_count = mesh.shape["feat"]
    cores = 2
    chips = feat_count // cores
    data_spec = P("ens", None, "feat")
    mean_spec = P("ens", "feat")
    prec_spec = P(("ens", "feat"))
    factor_spec = P(("ens", "feat"), None)

    def local_steps(particles, target_mean, precision, low_factor):
        num_ens, num_part, loc_feat = particles.shape
        rank = low_factor.shape[1]
        half = num_part // 2
        core_rows = half // cores
        piece = core_rows // chips
        width = 2 * half + 2 * rank
        bandwidth = 2.0 * loc_feat * feat_count
        step_size = 0.25 * loc_feat * feat_count
        prec_row = precision.reshape(1, loc_feat)
        low_t = low_factor.T
        f32, bf16 = jnp.float32, jnp.bfloat16
        vmem = pl.BlockSpec(memory_space=pltpu.VMEM)
        anyspace = pl.BlockSpec(memory_space=pl.ANY)
        dma = pltpu.SemaphoreType.DMA
        nsem = 2 * num_ens * chips
        theta, kern, proj, sums = pl.pallas_call(
            functools.partial(exchange_kernel, cores, chips),
            out_shape=(
                jax.ShapeDtypeStruct((num_ens, num_part, loc_feat), f32),
                jax.ShapeDtypeStruct((num_part, num_part), bf16),
                jax.ShapeDtypeStruct((num_part, 2 * rank), bf16),
                jax.ShapeDtypeStruct((num_part, 128), f32),
            ),
            in_specs=[anyspace, vmem, vmem, vmem],
            out_specs=(vmem, vmem, vmem, vmem),
            scratch_shapes=[
                pltpu.VMEM((num_ens, num_part, loc_feat), bf16),
                pltpu.VMEM((2 * rank, loc_feat), bf16),
                pltpu.VMEM((num_part, num_part), bf16),
                pltpu.VMEM((num_part, 2 * rank), bf16),
                pltpu.VMEM((num_part, 128), f32),
                pltpu.VMEM((num_ens, num_part, 2 * rank), f32),
                pltpu.VMEM((num_part, num_part), f32),
                pltpu.VMEM((num_ens, half, width), f32),
                pltpu.VMEM((num_ens, 8, half), f32),
                pltpu.VMEM((num_ens, core_rows, width), f32),
                pltpu.VMEM((num_ens, 8, half), f32),
                pltpu.VMEM((num_ens, core_rows, width), f32),
                pltpu.VMEM((num_ens, 8, half), f32),
                pltpu.VMEM((num_ens, chips - 1, piece, width), f32),
                pltpu.VMEM((num_ens, chips - 1, 8, half), f32),
                pltpu.VMEM((num_ens, half, width), bf16),
                pltpu.VMEM((num_ens, feat_count, 8, half), f32),
                dma((num_ens * CHUNKS,)),
                dma((2 * num_ens,)), dma((2 * num_ens,)),
                dma((nsem,)), dma((nsem,)),
                dma((nsem,)), dma((nsem,)),
                dma((nsem,)), dma((nsem,)),
            ],
            compiler_params=pltpu.CompilerParams(
                collective_id=0, has_side_effects=True, vmem_limit_bytes=VMEM_LIMIT),
            name="exchange",
        )(particles, target_mean, prec_row, low_t)
        tiles = loc_feat // TILE
        return pl.pallas_call(
            functools.partial(final_kernel, bandwidth, step_size),
            out_shape=jax.ShapeDtypeStruct((num_ens, num_part, loc_feat), f32),
            in_specs=[vmem] * 7,
            out_specs=anyspace,
            scratch_shapes=[pltpu.VMEM((tiles, num_part, TILE), f32), dma((num_ens - 1 + tiles,))],
            compiler_params=pltpu.CompilerParams(vmem_limit_bytes=FINAL_LIMIT),
            name="final_update",
        )(theta, kern, proj, sums, target_mean, prec_row, low_t)

    return jax.shard_map(local_steps, mesh=mesh, in_specs=(data_spec, mean_spec, prec_spec, factor_spec),
                         out_specs=data_spec, check_vma=False)
```

```python
import functools

import jax
import jax.numpy as jnp
from jax import lax
from jax.experimental import pallas as pl
from jax.experimental.pallas import tpu as pltpu
from jax.sharding import PartitionSpec as P

NUM_STEPS = 3
MESH = pl.DeviceIdType.MESH
NT = (((1,), (1,)), ((), ()))
CHUNKS = 4
TILE = 512
LANES = 128
VMEM_LIMIT = 40 * 1024 * 1024
FINAL_LIMIT = 20 * 1024 * 1024


def dot_nt(a, b):
    return lax.dot_general(a, b, NT, preferred_element_type=jnp.float32)


def advance(th, kern, yn, sums, step_size, num_part):
    drive = jnp.dot(kern[...], yn, preferred_element_type=jnp.float32)
    srow = jnp.concatenate([sums[...]] * (th.shape[1] // LANES), axis=1)
    return th + step_size * ((srow * th - drive) / num_part)


def exchange_kernel(cores, chips, part_hbm, mean_hbm, prec_hbm, low_hbm,
                    theta, kern1, sums1, yn1,
                    theta_bf, mean, prec, factor, factor2, kern0, sums0, yn0, proj, proj_part, gram,
                    gbuf, gsib, acc, gpeer, kbuf, qbuf, qsib, qacc, qpeer, qall, dbuf, dpeer, sbuf,
                    load_sem, small_sem, g1s, g1r, g2s, g2r, g3s, g3r,
                    q1s, q1r, q2s, q2r, q3s, q3r, ds, dr, t3s, t3r):
    num_ens, num_part, loc_feat = theta.shape
    half = num_part // 2
    group = cores * chips
    core_rows = half // cores
    piece = core_rows // chips
    bandwidth = 2.0 * loc_feat * group
    step_size = 0.25 * loc_feat * group
    kern, sums, yn = (kern0, kern1), (sums0, sums1), (yn0, yn1)

    me = lax.axis_index("feat")
    core = lax.rem(me, cores)
    chip = lax.div(me, cores)
    sibling = chip * cores + (1 - core)
    my_rows = pl.ds(pl.multiple_of(core * core_rows, core_rows), core_rows)
    sib_rows = pl.ds(pl.multiple_of((1 - core) * core_rows, core_rows), core_rows)
    first_row = pl.multiple_of(core * core_rows + chip * piece, piece)
    my_piece = pl.ds(first_row, piece)
    own_rows = pl.ds(pl.multiple_of(chip * piece, piece), piece)

    def chip_at(offset):
        return lax.rem(chip + offset, chips)

    def peer(offset):
        return chip_at(offset) * cores + core

    def remote(src, dst, send, recv, dev):
        return pltpu.make_async_remote_copy(src_ref=src, dst_ref=dst, send_sem=send, recv_sem=recv,
                                            device_id={"feat": dev}, device_id_type=MESH)

    far_first = sorted(range(1, chips), key=lambda k: -min(k, chips - k))
    near_first = far_first[::-1]

    rows = num_part // CHUNKS
    smalls = [pltpu.make_async_copy(a, b, small_sem.at[i])
              for i, (a, b) in enumerate(((low_hbm, factor), (mean_hbm, mean), (prec_hbm, prec)))]
    for c in smalls:
        c.start()
    loads = {}
    for e in range(num_ens):
        for c in range(CHUNKS):
            loads[e, c] = pltpu.make_async_copy(part_hbm.at[e, pl.ds(c * rows, rows)],
                                                theta.at[e, pl.ds(c * rows, rows)], load_sem.at[e * CHUNKS + c])
    for c in range(CHUNKS):
        loads[0, c].start()

    barrier = pltpu.get_barrier_semaphore()
    for offset in range(1, group):
        pl.semaphore_signal(barrier, inc=1, device_id={"feat": lax.rem(me + offset, group)}, device_id_type=MESH)

    for c in smalls:
        c.wait()
    factor2[...] = jnp.concatenate([factor[...], factor[...]], axis=0)
    rank2 = factor2.shape[0]
    rank = rank2 // 2
    lane_low = lax.broadcasted_iota(jnp.int32, (half, rank2), 1) < rank
    row_id = lax.broadcasted_iota(jnp.int32, (half, half), 0)
    col_id = lax.broadcasted_iota(jnp.int32, (half, half), 1)

    def g1(e):
        return remote(gbuf.at[e, sib_rows], gsib.at[e], g1s.at[e], g1r.at[e], sibling)

    def q1(e):
        return remote(qbuf.at[e, sib_rows], qsib.at[e], q1s.at[e], q1r.at[e], sibling)

    def dg(e, o):
        i = e * group + o
        return remote(dbuf.at[e], dpeer.at[e, o - 1], ds.at[i], dr.at[i], lax.rem(me + o, group))

    def to_owner(src, dst, send, recv, e, k):
        i = e * chips + k
        return remote(src.at[e, pl.ds(pl.multiple_of(chip_at(k) * piece, piece), piece)], dst.at[e, k - 1],
                      send.at[i], recv.at[i], peer(k))

    def g2(e, k):
        return to_owner(acc, gpeer, g2s, g2r, e, k)

    def q2(e, k):
        return to_owner(qacc, qpeer, q2s, q2r, e, k)

    def rows_of(owner_core, owner_chip):
        return pl.ds(pl.multiple_of(owner_core * core_rows + owner_chip * piece, piece), piece)

    def core_of(other):
        return (1 - core) if other else core

    def out_of(buf, index, send, recv, e, k, other):
        i = 2 * (e * chips + k) + other
        return remote(buf.at[e, index], buf.at[e, index], send.at[i], recv.at[i], chip_at(k) * cores + core_of(other))

    def into(buf, lines, send, recv, e, k, other):
        i = 2 * (e * chips + k) + other
        src, src_core = chip_at(chips - k), core_of(other)
        index = src * cores + src_core if lines else rows_of(src_core, src)
        return remote(buf.at[e, index], buf.at[e, index], send.at[i], recv.at[i], src * cores + src_core)

    others = [(k, other) for k in far_first for other in (0, 1)] + [(0, 1)]

    def spread(key, buf, index, send_sem, recv_sem, e):
        for k, other in others:
            send((key, e), out_of(buf, index, send_sem, recv_sem, e, k, other))

    def gathered(buf, lines, send_sem, recv_sem, e):
        for k, other in others:
            into(buf, lines, send_sem, recv_sem, e, k, other).wait_recv()

    pending = {}

    def send(key, *copies):
        for c in copies:
            c.start()
        pending.setdefault(key, []).extend(copies)

    def drain(key):
        for c in pending.pop(key, []):
            c.wait_send()

    def first_rows(e):
        for c in range(CHUNKS):
            loads[e, c].wait()
            if e + 1 < num_ens:
                loads[e + 1, c].start()
            sl = pl.ds(c * rows, rows)
            th = theta[e, sl, :]
            theta_bf[e, sl, :] = th.astype(jnp.bfloat16)
            xb = (th - mean[e:e + 1, :]).astype(jnp.bfloat16)
            proj_part[e, sl, :] = dot_nt(xb, factor2[...])

    def send_q(e):
        qbuf[e] = jnp.where(lane_low, proj_part[e, 0:half, :], proj_part[e, half:, :])
        send(("q1", e), q1(e))

    def gram_and_send(e):
        gram[...] = dot_nt(theta_bf[e], theta_bf[e])
        g00 = gram[0:half, 0:half]
        g11 = gram[half:, half:]
        gbuf[e, :, 0:half] = jnp.where(col_id >= row_id, g00, g11)
        gbuf[e, :, half:2 * half] = gram[0:half, half:]
        send(("g1", e), g1(e))
        d0 = jnp.sum(jnp.where(col_id == row_id, g00, 0.0), axis=0, keepdims=True)
        d1 = jnp.sum(jnp.where(col_id == row_id, g11, 0.0), axis=0, keepdims=True)
        pack_lines(dbuf.at[e], d0, d1)
        for o in range(1, group):
            send(("d", e), dg(e, o))

    def pack_lines(ref, a, b):
        n = half // LANES
        for i in range(n):
            ref[i:i + 1, :] = a[:, i * LANES:(i + 1) * LANES]
            ref[n + i:n + i + 1, :] = b[:, i * LANES:(i + 1) * LANES]

    def stage_q1(e):
        q1(e).wait_recv()
        qacc[e] = qbuf[e, my_rows, :] + qsib[e]
        for k in far_first:
            send(("q2", e), q2(e, k))

    def stage_g1(e):
        g1(e).wait_recv()
        acc[e] = gbuf[e, my_rows, :] + gsib[e]
        for k in far_first:
            send(("g2", e), g2(e, k))

    def stage_q2(e):
        own = qacc[e, own_rows, :]
        for k in range(1, chips):
            q2(e, k).wait_recv()
            own = own + qpeer[e, k - 1]
        qall[e, my_piece, :] = own.astype(jnp.bfloat16)
        spread("q3", qall, my_piece, q3s, q3r, e)

    def stage_g2(e):
        tot = dbuf[e]
        for o in range(1, group):
            dg(e, o).wait_recv()
            tot = tot + dpeer[e, o - 1]
        n = half // LANES
        l0 = jnp.concatenate([tot[i:i + 1, :] for i in range(n)], axis=1)
        l1 = jnp.concatenate([tot[n + i:n + i + 1, :] for i in range(n)], axis=1)
        col = lax.broadcasted_iota(jnp.int32, (piece, half), 1)
        row = lax.broadcasted_iota(jnp.int32, (piece, half), 0) + first_row
        on = col == row
        up = col >= row
        c0 = jnp.sum(jnp.where(on, l0, 0.0), axis=1, keepdims=True)
        c1 = jnp.sum(jnp.where(on, l1, 0.0), axis=1, keepdims=True)
        diag_t = jnp.where(up, c0 + l0, c1 + l1)
        diag_o = c0 + l1
        own = acc[e, own_rows, :]
        for k in near_first:
            g2(e, k).wait_recv()
            own = own + gpeer[e, k - 1]
        k_t = jnp.where(on, 1.0, jnp.exp(-jnp.maximum(diag_t - 2.0 * own[:, 0:half], 0.0) / bandwidth))
        k_o = jnp.exp(-jnp.maximum(diag_o - 2.0 * own[:, half:], 0.0) / bandwidth)
        kbuf[e, my_piece, 0:half] = k_t.astype(jnp.bfloat16)
        kbuf[e, my_piece, half:] = k_o.astype(jnp.bfloat16)
        spread("g3", kbuf, my_piece, g3s, g3r, e)
        low = col < row
        row0 = jnp.sum(jnp.where(up, k_t, 0.0) + k_o, axis=1, keepdims=True)
        row1 = jnp.sum(jnp.where(low, k_t, 0.0), axis=1, keepdims=True) + 1.0
        s0 = jnp.sum(jnp.where(col > row, k_t, 0.0) + jnp.where(on, row0, 0.0), axis=0, keepdims=True)
        s1 = jnp.sum(jnp.where(low, k_t, 0.0) + k_o + jnp.where(on, row1, 0.0), axis=0, keepdims=True)
        pack_lines(sbuf.at[e, me], s0, s1)
        spread("t3", sbuf, me, t3s, t3r, e)

    def stage_y(e, t0, t1):
        if t0 == 0:
            gathered(qall, False, q3s, q3r, e)
            pj = qall[e].astype(jnp.float32)
            proj[e, 0:half, :] = jnp.where(lane_low, pj, 0.0).astype(jnp.bfloat16)
            proj[e, half:, :] = jnp.where(lane_low, 0.0, pj).astype(jnp.bfloat16)
        for t in range(t0, t1):
            sl = pl.ds(t * TILE, TILE)
            th = theta[e, :, sl]
            low = jnp.dot(proj[e], factor2[:, sl], preferred_element_type=jnp.float32)
            yn[e][:, sl] = ((th - mean[e:e + 1, sl]) * prec[0:1, sl] + low + (2.0 / bandwidth) * th).astype(jnp.bfloat16)

    def unpack(e):
        gathered(kbuf, False, g3s, g3r, e)
        for key in ("g1", "q1", "g2", "q2", "g3", "q3", "d", "t3"):
            drain((key, e))
        kern_ref, sums_ref = kern[e], sums[e]
        t = kbuf[e, :, 0:half].astype(jnp.float32)
        tt = t.T
        kern_ref[0:half, 0:half] = jnp.where(col_id >= row_id, t, tt).astype(jnp.bfloat16)
        kern_ref[half:, half:] = jnp.where(col_id <= row_id, t, tt).astype(jnp.bfloat16)
        ko = kbuf[e, :, half:]
        kern_ref[0:half, half:] = ko
        kern_ref[half:, 0:half] = ko.astype(jnp.float32).T.astype(jnp.bfloat16)
        gathered(sbuf, True, t3s, t3r, e)
        tot = sbuf[e, 0]
        for o in range(1, group):
            tot = tot + sbuf[e, o]
        tot = (2.0 / bandwidth) * tot
        for q in range(num_part // LANES):
            sums_ref[q * LANES:(q + 1) * LANES, :] = jnp.broadcast_to(tot[q:q + 1, :], (LANES, LANES)).T

    def update(e, last, t0, t1):
        for t in range(t0, t1):
            sl = pl.ds(t * TILE, TILE)
            new = advance(theta[e, :, sl], kern[e], yn[e][:, sl], sums[e], step_size, num_part)
            theta[e, :, sl] = new
            if last:
                continue
            theta_bf[e, :, sl] = new.astype(jnp.bfloat16)
            xb = (new - mean[e:e + 1, sl]).astype(jnp.bfloat16)
            part = dot_nt(xb, factor2[:, sl])
            if t == 0:
                proj_part[e] = part
            else:
                proj_part[e] += part

    first_rows(0)
    pl.semaphore_wait(barrier, group - 1)
    send_q(0)
    gram_and_send(0)
    stage_q1(0)
    first_rows(1)
    send_q(1)
    stage_g1(0)
    gram_and_send(1)
    stage_q1(1)
    stage_q2(0)
    stage_g1(1)
    stage_q2(1)
    stage_g2(0)
    stage_y(0, 0, 4)
    stage_g2(1)
    stage_y(1, 0, 4)
    unpack(0)
    update(0, False, 0, 4)
    send_q(0)
    gram_and_send(0)
    stage_q1(0)
    unpack(1)
    stage_g1(0)
    update(1, False, 0, 4)
    send_q(1)
    stage_q2(0)
    gram_and_send(1)
    stage_q1(1)
    stage_g1(1)
    stage_q2(1)
    stage_g2(0)
    stage_y(0, 0, 4)
    stage_g2(1)
    stage_y(1, 0, 4)
    unpack(0)
    update(0, False, 0, 4)
    send_q(0)
    gram_and_send(0)
    stage_q1(0)
    unpack(1)
    stage_g1(0)
    update(1, False, 0, 4)
    send_q(1)
    stage_q2(0)
    gram_and_send(1)
    stage_q1(1)
    stage_g1(1)
    stage_q2(1)
    stage_g2(0)
    stage_y(0, 0, 4)
    stage_g2(1)
    stage_y(1, 0, 4)
    unpack(0)
    update(0, True, 0, 4)
    unpack(1)
    for key in list(pending):
        drain(key)


def final_kernel(step_size, theta, kern, sums, yn, out_hbm, done, store_sem):
    num_ens, num_part, loc_feat = theta.shape
    stores = []
    for e in range(num_ens - 1):
        stores.append(pltpu.make_async_copy(theta.at[e], out_hbm.at[e], store_sem.at[e]))
        stores[-1].start()
    e = num_ens - 1
    for t in range(loc_feat // TILE):
        sl = pl.ds(t * TILE, TILE)
        done[t] = advance(theta[e, :, sl], kern, yn[:, sl], sums, step_size, num_part)
        stores.append(pltpu.make_async_copy(done.at[t], out_hbm.at[e, :, sl], store_sem.at[e + t]))
        stores[-1].start()
    for st in stores:
        st.wait()


def solution(mesh):
    feat_count = mesh.shape["feat"]
    cores = 2
    chips = feat_count // cores
    data_spec = P("ens", None, "feat")
    mean_spec = P("ens", "feat")
    prec_spec = P(("ens", "feat"))
    factor_spec = P(("ens", "feat"), None)

    def local_steps(particles, target_mean, precision, low_factor):
        num_ens, num_part, loc_feat = particles.shape
        rank = low_factor.shape[1]
        half = num_part // 2
        core_rows = half // cores
        piece = core_rows // chips
        lines = num_part // LANES
        step_size = 0.25 * loc_feat * feat_count
        prec_row = precision.reshape(1, loc_feat)
        low_t = low_factor.T
        f32, bf16 = jnp.float32, jnp.bfloat16
        vmem = pl.BlockSpec(memory_space=pltpu.VMEM)
        hbm = pl.BlockSpec(memory_space=pltpu.HBM)
        dma = pltpu.SemaphoreType.DMA
        nsem = num_ens * chips

        def sems(count, pairs):
            return [dma((count,))] * (2 * pairs)

        theta, kern, sums, yn = pl.pallas_call(
            functools.partial(exchange_kernel, cores, chips),
            out_shape=(
                jax.ShapeDtypeStruct((num_ens, num_part, loc_feat), f32),
                jax.ShapeDtypeStruct((num_part, num_part), bf16),
                jax.ShapeDtypeStruct((num_part, LANES), f32),
                jax.ShapeDtypeStruct((num_part, loc_feat), bf16),
            ),
            in_specs=[hbm] * 4,
            out_specs=(vmem,) * 4,
            scratch_shapes=[
                pltpu.VMEM((num_ens, num_part, loc_feat), bf16),
                pltpu.VMEM((num_ens, loc_feat), f32),
                pltpu.VMEM((1, loc_feat), f32),
                pltpu.VMEM((rank, loc_feat), bf16),
                pltpu.VMEM((2 * rank, loc_feat), bf16),
                pltpu.VMEM((num_part, num_part), bf16),
                pltpu.VMEM((num_part, LANES), f32),
                pltpu.VMEM((num_part, loc_feat), bf16),
                pltpu.VMEM((num_ens, num_part, 2 * rank), bf16),
                pltpu.VMEM((num_ens, num_part, 2 * rank), f32),
                pltpu.VMEM((num_part, num_part), f32),
                pltpu.VMEM((num_ens, half, num_part), f32),
                pltpu.VMEM((num_ens, core_rows, num_part), f32),
                pltpu.VMEM((num_ens, core_rows, num_part), f32),
                pltpu.VMEM((num_ens, chips - 1, piece, num_part), f32),
                pltpu.VMEM((num_ens, half, num_part), bf16),
                pltpu.VMEM((num_ens, half, 2 * rank), f32),
                pltpu.VMEM((num_ens, core_rows, 2 * rank), f32),
                pltpu.VMEM((num_ens, core_rows, 2 * rank), f32),
                pltpu.VMEM((num_ens, chips - 1, piece, 2 * rank), f32),
                pltpu.VMEM((num_ens, half, 2 * rank), bf16),
                pltpu.VMEM((num_ens, lines, LANES), f32),
                pltpu.VMEM((num_ens, feat_count - 1, lines, LANES), f32),
                pltpu.VMEM((num_ens, feat_count, lines, LANES), f32),
                dma((num_ens * CHUNKS,)),
                dma((3,)),
                *sems(num_ens, 1), *sems(nsem, 1), *sems(2 * nsem, 1),
                *sems(num_ens, 1), *sems(nsem, 1), *sems(2 * nsem, 1),
                *sems(num_ens * feat_count, 1), *sems(2 * nsem, 1),
            ],
            compiler_params=pltpu.CompilerParams(
                collective_id=0, has_side_effects=True, vmem_limit_bytes=VMEM_LIMIT),
            name="exchange",
        )(particles, *[pltpu.with_memory_space_constraint(v, pltpu.HBM) for v in (target_mean, prec_row, low_t)])
        tiles = loc_feat // TILE
        return pl.pallas_call(
            functools.partial(final_kernel, step_size),
            out_shape=jax.ShapeDtypeStruct((num_ens, num_part, loc_feat), f32),
            in_specs=[vmem] * 4,
            out_specs=hbm,
            scratch_shapes=[pltpu.VMEM((tiles, num_part, TILE), f32), dma((num_ens - 1 + tiles,))],
            compiler_params=pltpu.CompilerParams(vmem_limit_bytes=FINAL_LIMIT),
            name="final_update",
        )(theta, kern, sums, yn)

    return jax.shard_map(local_steps, mesh=mesh, in_specs=(data_spec, mean_spec, prec_spec, factor_spec),
                         out_specs=data_spec, check_vma=False)
```

```python
import functools

import jax
import jax.numpy as jnp
from jax import lax
from jax.experimental import pallas as pl
from jax.experimental.pallas import tpu as pltpu
from jax.sharding import PartitionSpec as P

NUM_STEPS = 3
MESH = pl.DeviceIdType.MESH
NT = (((1,), (1,)), ((), ()))
CHUNKS = 4
TILE = 512
LANES = 128
VMEM_LIMIT = 40 * 1024 * 1024
FINAL_LIMIT = 20 * 1024 * 1024


def dot_nt(a, b):
    return lax.dot_general(a, b, NT, preferred_element_type=jnp.float32)


def advance(th, kern, yn, sums, step_size, num_part):
    drive = jnp.dot(kern[...], yn, preferred_element_type=jnp.float32)
    srow = jnp.concatenate([sums[...]] * (th.shape[1] // LANES), axis=1)
    return th + step_size * ((srow * th - drive) / num_part)


def exchange_kernel(cores, chips, part_hbm, mean_hbm, prec_hbm, low_hbm,
                    theta, kern1, sums1, yn1,
                    theta_bf, mean, prec, factor, factor2, kern0, sums0, yn0, proj, proj_part, gram,
                    gbuf, gsib, acc, gpeer, kbuf, qbuf, qsib, qacc, qpeer, qall, dbuf, dpeer, sbuf,
                    load_sem, small_sem, g1s, g1r, g2s, g2r, g3s, g3r,
                    q1s, q1r, q2s, q2r, q3s, q3r, ds, dr, t3s, t3r):
    num_ens, num_part, loc_feat = theta.shape
    half = num_part // 2
    group = cores * chips
    core_rows = half // cores
    piece = core_rows // chips
    bandwidth = 2.0 * loc_feat * group
    step_size = 0.25 * loc_feat * group
    kern, sums, yn = (kern0, kern1), (sums0, sums1), (yn0, yn1)

    me = lax.axis_index("feat")
    core = lax.rem(me, cores)
    chip = lax.div(me, cores)
    sibling = chip * cores + (1 - core)
    my_rows = pl.ds(pl.multiple_of(core * core_rows, core_rows), core_rows)
    sib_rows = pl.ds(pl.multiple_of((1 - core) * core_rows, core_rows), core_rows)
    first_row = pl.multiple_of(core * core_rows + chip * piece, piece)
    my_piece = pl.ds(first_row, piece)
    own_rows = pl.ds(pl.multiple_of(chip * piece, piece), piece)

    def chip_at(offset):
        return lax.rem(chip + offset, chips)

    def peer(offset):
        return chip_at(offset) * cores + core

    def remote(src, dst, send, recv, dev):
        return pltpu.make_async_remote_copy(src_ref=src, dst_ref=dst, send_sem=send, recv_sem=recv,
                                            device_id={"feat": dev}, device_id_type=MESH)

    far_first = sorted(range(1, chips), key=lambda k: -min(k, chips - k))
    near_first = far_first[::-1]

    rows = num_part // CHUNKS
    smalls = [pltpu.make_async_copy(a, b, small_sem.at[i])
              for i, (a, b) in enumerate(((low_hbm, factor), (mean_hbm, mean), (prec_hbm, prec)))]
    for c in smalls:
        c.start()
    loads = {}
    for e in range(num_ens):
        for c in range(CHUNKS):
            loads[e, c] = pltpu.make_async_copy(part_hbm.at[e, pl.ds(c * rows, rows)],
                                                theta.at[e, pl.ds(c * rows, rows)], load_sem.at[e * CHUNKS + c])
    for c in range(CHUNKS):
        loads[0, c].start()

    barrier = pltpu.get_barrier_semaphore()
    for offset in range(1, group):
        pl.semaphore_signal(barrier, inc=1, device_id={"feat": lax.rem(me + offset, group)}, device_id_type=MESH)

    for c in smalls:
        c.wait()
    factor2[...] = jnp.concatenate([factor[...], factor[...]], axis=0)
    rank2 = factor2.shape[0]
    rank = rank2 // 2
    lane_low = lax.broadcasted_iota(jnp.int32, (half, rank2), 1) < rank
    row_id = lax.broadcasted_iota(jnp.int32, (half, half), 0)
    col_id = lax.broadcasted_iota(jnp.int32, (half, half), 1)

    def g1(e):
        return remote(gbuf.at[e, sib_rows], gsib.at[e], g1s.at[e], g1r.at[e], sibling)

    def q1(e):
        return remote(qbuf.at[e, sib_rows], qsib.at[e], q1s.at[e], q1r.at[e], sibling)

    def dg(e, o):
        i = e * group + o
        return remote(dbuf.at[e], dpeer.at[e, o - 1], ds.at[i], dr.at[i], lax.rem(me + o, group))

    def to_owner(src, dst, send, recv, e, k):
        i = e * chips + k
        return remote(src.at[e, pl.ds(pl.multiple_of(chip_at(k) * piece, piece), piece)], dst.at[e, k - 1],
                      send.at[i], recv.at[i], peer(k))

    def g2(e, k):
        return to_owner(acc, gpeer, g2s, g2r, e, k)

    def q2(e, k):
        return to_owner(qacc, qpeer, q2s, q2r, e, k)

    def rows_of(owner_core, owner_chip):
        return pl.ds(pl.multiple_of(owner_core * core_rows + owner_chip * piece, piece), piece)

    def core_of(other):
        return (1 - core) if other else core

    def out_of(buf, index, send, recv, e, k, other):
        i = 2 * (e * chips + k) + other
        return remote(buf.at[e, index], buf.at[e, index], send.at[i], recv.at[i], chip_at(k) * cores + core_of(other))

    def into(buf, lines, send, recv, e, k, other):
        i = 2 * (e * chips + k) + other
        src, src_core = chip_at(chips - k), core_of(other)
        index = src * cores + src_core if lines else rows_of(src_core, src)
        return remote(buf.at[e, index], buf.at[e, index], send.at[i], recv.at[i], src * cores + src_core)

    others = [(k, other) for k in far_first for other in (0, 1)] + [(0, 1)]

    def spread(key, buf, index, send_sem, recv_sem, e):
        for k, other in others:
            send((key, e), out_of(buf, index, send_sem, recv_sem, e, k, other))

    def gathered(buf, lines, send_sem, recv_sem, e):
        for k, other in others:
            into(buf, lines, send_sem, recv_sem, e, k, other).wait_recv()

    pending = {}

    def send(key, *copies):
        for c in copies:
            c.start()
        pending.setdefault(key, []).extend(copies)

    def drain(key):
        for c in pending.pop(key, []):
            c.wait_send()

    def first_rows(e):
        for c in range(CHUNKS):
            loads[e, c].wait()
            if e + 1 < num_ens:
                loads[e + 1, c].start()
            sl = pl.ds(c * rows, rows)
            th = theta[e, sl, :]
            theta_bf[e, sl, :] = th.astype(jnp.bfloat16)
            xb = (th - mean[e:e + 1, :]).astype(jnp.bfloat16)
            proj_part[e, sl, :] = dot_nt(xb, factor2[...])

    def send_q(e):
        qbuf[e] = jnp.where(lane_low, proj_part[e, 0:half, :], proj_part[e, half:, :])
        send(("q1", e), q1(e))

    def gram_and_send(e):
        gram[...] = dot_nt(theta_bf[e], theta_bf[e])
        g00 = gram[0:half, 0:half]
        g11 = gram[half:, half:]
        gbuf[e, :, 0:half] = jnp.where(col_id >= row_id, g00, g11)
        gbuf[e, :, half:2 * half] = gram[0:half, half:]
        send(("g1", e), g1(e))
        d0 = jnp.sum(jnp.where(col_id == row_id, g00, 0.0), axis=0, keepdims=True)
        d1 = jnp.sum(jnp.where(col_id == row_id, g11, 0.0), axis=0, keepdims=True)
        pack_lines(dbuf.at[e], d0, d1)
        for o in range(1, group):
            send(("d", e), dg(e, o))

    def pack_lines(ref, a, b):
        n = half // LANES
        for i in range(n):
            ref[i:i + 1, :] = a[:, i * LANES:(i + 1) * LANES]
            ref[n + i:n + i + 1, :] = b[:, i * LANES:(i + 1) * LANES]

    def stage_q1(e):
        q1(e).wait_recv()
        qacc[e] = qbuf[e, my_rows, :] + qsib[e]
        for k in far_first:
            send(("q2", e), q2(e, k))

    def stage_g1(e):
        g1(e).wait_recv()
        acc[e] = gbuf[e, my_rows, :] + gsib[e]
        for k in far_first:
            send(("g2", e), g2(e, k))

    def stage_q2(e):
        own = qacc[e, own_rows, :]
        for k in range(1, chips):
            q2(e, k).wait_recv()
            own = own + qpeer[e, k - 1]
        qall[e, my_piece, :] = own.astype(jnp.bfloat16)
        spread("q3", qall, my_piece, q3s, q3r, e)

    def stage_g2(e):
        tot = dbuf[e]
        for o in range(1, group):
            dg(e, o).wait_recv()
            tot = tot + dpeer[e, o - 1]
        n = half // LANES
        l0 = jnp.concatenate([tot[i:i + 1, :] for i in range(n)], axis=1)
        l1 = jnp.concatenate([tot[n + i:n + i + 1, :] for i in range(n)], axis=1)
        col = lax.broadcasted_iota(jnp.int32, (piece, half), 1)
        row = lax.broadcasted_iota(jnp.int32, (piece, half), 0) + first_row
        on = col == row
        up = col >= row
        c0 = jnp.sum(jnp.where(on, l0, 0.0), axis=1, keepdims=True)
        c1 = jnp.sum(jnp.where(on, l1, 0.0), axis=1, keepdims=True)
        diag_t = jnp.where(up, c0 + l0, c1 + l1)
        diag_o = c0 + l1
        own = acc[e, own_rows, :]
        for k in near_first:
            g2(e, k).wait_recv()
            own = own + gpeer[e, k - 1]
        k_t = jnp.where(on, 1.0, jnp.exp(-jnp.maximum(diag_t - 2.0 * own[:, 0:half], 0.0) / bandwidth))
        k_o = jnp.exp(-jnp.maximum(diag_o - 2.0 * own[:, half:], 0.0) / bandwidth)
        kbuf[e, my_piece, 0:half] = k_t.astype(jnp.bfloat16)
        kbuf[e, my_piece, half:] = k_o.astype(jnp.bfloat16)
        spread("g3", kbuf, my_piece, g3s, g3r, e)
        low = col < row
        row0 = jnp.sum(jnp.where(up, k_t, 0.0) + k_o, axis=1, keepdims=True)
        row1 = jnp.sum(jnp.where(low, k_t, 0.0), axis=1, keepdims=True) + 1.0
        s0 = jnp.sum(jnp.where(col > row, k_t, 0.0) + jnp.where(on, row0, 0.0), axis=0, keepdims=True)
        s1 = jnp.sum(jnp.where(low, k_t, 0.0) + k_o + jnp.where(on, row1, 0.0), axis=0, keepdims=True)
        pack_lines(sbuf.at[e, me], s0, s1)
        spread("t3", sbuf, me, t3s, t3r, e)

    def stage_y(e, t0, t1):
        if t0 == 0:
            gathered(qall, False, q3s, q3r, e)
            pj = qall[e].astype(jnp.float32)
            proj[e, 0:half, :] = jnp.where(lane_low, pj, 0.0).astype(jnp.bfloat16)
            proj[e, half:, :] = jnp.where(lane_low, 0.0, pj).astype(jnp.bfloat16)
        for t in range(t0, t1):
            sl = pl.ds(t * TILE, TILE)
            th = theta[e, :, sl]
            low = jnp.dot(proj[e], factor2[:, sl], preferred_element_type=jnp.float32)
            yn[e][:, sl] = ((th - mean[e:e + 1, sl]) * prec[0:1, sl] + low + (2.0 / bandwidth) * th).astype(jnp.bfloat16)

    def unpack(e):
        gathered(kbuf, False, g3s, g3r, e)
        for key in ("g1", "q1", "g2", "q2", "g3", "q3", "d", "t3"):
            drain((key, e))
        kern_ref, sums_ref = kern[e], sums[e]
        t = kbuf[e, :, 0:half].astype(jnp.float32)
        tt = t.T
        kern_ref[0:half, 0:half] = jnp.where(col_id >= row_id, t, tt).astype(jnp.bfloat16)
        kern_ref[half:, half:] = jnp.where(col_id <= row_id, t, tt).astype(jnp.bfloat16)
        ko = kbuf[e, :, half:]
        kern_ref[0:half, half:] = ko
        kern_ref[half:, 0:half] = ko.astype(jnp.float32).T.astype(jnp.bfloat16)
        gathered(sbuf, True, t3s, t3r, e)
        tot = sbuf[e, 0]
        for o in range(1, group):
            tot = tot + sbuf[e, o]
        tot = (2.0 / bandwidth) * tot
        for q in range(num_part // LANES):
            sums_ref[q * LANES:(q + 1) * LANES, :] = jnp.broadcast_to(tot[q:q + 1, :], (LANES, LANES)).T

    def update(e, last, t0, t1):
        for t in range(t0, t1):
            sl = pl.ds(t * TILE, TILE)
            new = advance(theta[e, :, sl], kern[e], yn[e][:, sl], sums[e], step_size, num_part)
            theta[e, :, sl] = new
            if last:
                continue
            theta_bf[e, :, sl] = new.astype(jnp.bfloat16)
            xb = (new - mean[e:e + 1, sl]).astype(jnp.bfloat16)
            part = dot_nt(xb, factor2[:, sl])
            if t == 0:
                proj_part[e] = part
            else:
                proj_part[e] += part

    first_rows(0)
    pl.semaphore_wait(barrier, group - 1)
    send_q(0)
    gram_and_send(0)
    stage_q1(0)
    first_rows(1)
    send_q(1)
    stage_g1(0)
    gram_and_send(1)
    stage_q1(1)
    stage_q2(0)
    stage_g1(1)
    stage_q2(1)
    stage_g2(0)
    stage_g2(1)
    stage_y(0, 0, 4)
    stage_y(1, 0, 4)
    unpack(0)
    update(0, False, 0, 4)
    send_q(0)
    gram_and_send(0)
    stage_q1(0)
    unpack(1)
    update(1, False, 0, 1)
    stage_g1(0)
    update(1, False, 1, 2)
    update(1, False, 2, 4)
    send_q(1)
    stage_q2(0)
    gram_and_send(1)
    stage_q1(1)
    stage_g1(1)
    stage_q2(1)
    stage_g2(0)
    stage_g2(1)
    stage_y(0, 0, 4)
    stage_y(1, 0, 4)
    unpack(0)
    update(0, False, 0, 4)
    send_q(0)
    gram_and_send(0)
    stage_q1(0)
    unpack(1)
    update(1, False, 0, 1)
    stage_g1(0)
    update(1, False, 1, 2)
    update(1, False, 2, 4)
    send_q(1)
    stage_q2(0)
    gram_and_send(1)
    stage_q1(1)
    stage_g1(1)
    stage_q2(1)
    stage_g2(0)
    stage_g2(1)
    stage_y(0, 0, 4)
    stage_y(1, 0, 4)
    unpack(0)
    update(0, True, 0, 4)
    unpack(1)
    for key in list(pending):
        drain(key)


def final_kernel(step_size, theta, kern, sums, yn, out_hbm, done, store_sem):
    num_ens, num_part, loc_feat = theta.shape
    stores = []
    for e in range(num_ens - 1):
        stores.append(pltpu.make_async_copy(theta.at[e], out_hbm.at[e], store_sem.at[e]))
        stores[-1].start()
    e = num_ens - 1
    for t in range(loc_feat // TILE):
        sl = pl.ds(t * TILE, TILE)
        done[t] = advance(theta[e, :, sl], kern, yn[:, sl], sums, step_size, num_part)
        stores.append(pltpu.make_async_copy(done.at[t], out_hbm.at[e, :, sl], store_sem.at[e + t]))
        stores[-1].start()
    for st in stores:
        st.wait()


def solution(mesh):
    feat_count = mesh.shape["feat"]
    cores = 2
    chips = feat_count // cores
    data_spec = P("ens", None, "feat")
    mean_spec = P("ens", "feat")
    prec_spec = P(("ens", "feat"))
    factor_spec = P(("ens", "feat"), None)

    def local_steps(particles, target_mean, precision, low_factor):
        num_ens, num_part, loc_feat = particles.shape
        rank = low_factor.shape[1]
        half = num_part // 2
        core_rows = half // cores
        piece = core_rows // chips
        lines = num_part // LANES
        step_size = 0.25 * loc_feat * feat_count
        prec_row = precision.reshape(1, loc_feat)
        low_t = low_factor.T
        f32, bf16 = jnp.float32, jnp.bfloat16
        vmem = pl.BlockSpec(memory_space=pltpu.VMEM)
        hbm = pl.BlockSpec(memory_space=pltpu.HBM)
        dma = pltpu.SemaphoreType.DMA
        nsem = num_ens * chips

        def sems(count, pairs):
            return [dma((count,))] * (2 * pairs)

        theta, kern, sums, yn = pl.pallas_call(
            functools.partial(exchange_kernel, cores, chips),
            out_shape=(
                jax.ShapeDtypeStruct((num_ens, num_part, loc_feat), f32),
                jax.ShapeDtypeStruct((num_part, num_part), bf16),
                jax.ShapeDtypeStruct((num_part, LANES), f32),
                jax.ShapeDtypeStruct((num_part, loc_feat), bf16),
            ),
            in_specs=[hbm] * 4,
            out_specs=(vmem,) * 4,
            scratch_shapes=[
                pltpu.VMEM((num_ens, num_part, loc_feat), bf16),
                pltpu.VMEM((num_ens, loc_feat), f32),
                pltpu.VMEM((1, loc_feat), f32),
                pltpu.VMEM((rank, loc_feat), bf16),
                pltpu.VMEM((2 * rank, loc_feat), bf16),
                pltpu.VMEM((num_part, num_part), bf16),
                pltpu.VMEM((num_part, LANES), f32),
                pltpu.VMEM((num_part, loc_feat), bf16),
                pltpu.VMEM((num_ens, num_part, 2 * rank), bf16),
                pltpu.VMEM((num_ens, num_part, 2 * rank), f32),
                pltpu.VMEM((num_part, num_part), f32),
                pltpu.VMEM((num_ens, half, num_part), f32),
                pltpu.VMEM((num_ens, core_rows, num_part), f32),
                pltpu.VMEM((num_ens, core_rows, num_part), f32),
                pltpu.VMEM((num_ens, chips - 1, piece, num_part), f32),
                pltpu.VMEM((num_ens, half, num_part), bf16),
                pltpu.VMEM((num_ens, half, 2 * rank), f32),
                pltpu.VMEM((num_ens, core_rows, 2 * rank), f32),
                pltpu.VMEM((num_ens, core_rows, 2 * rank), f32),
                pltpu.VMEM((num_ens, chips - 1, piece, 2 * rank), f32),
                pltpu.VMEM((num_ens, half, 2 * rank), bf16),
                pltpu.VMEM((num_ens, lines, LANES), f32),
                pltpu.VMEM((num_ens, feat_count - 1, lines, LANES), f32),
                pltpu.VMEM((num_ens, feat_count, lines, LANES), f32),
                dma((num_ens * CHUNKS,)),
                dma((3,)),
                *sems(num_ens, 1), *sems(nsem, 1), *sems(2 * nsem, 1),
                *sems(num_ens, 1), *sems(nsem, 1), *sems(2 * nsem, 1),
                *sems(num_ens * feat_count, 1), *sems(2 * nsem, 1),
            ],
            compiler_params=pltpu.CompilerParams(
                collective_id=0, has_side_effects=True, vmem_limit_bytes=VMEM_LIMIT),
            name="exchange",
        )(particles, *[pltpu.with_memory_space_constraint(v, pltpu.HBM) for v in (target_mean, prec_row, low_t)])
        tiles = loc_feat // TILE
        return pl.pallas_call(
            functools.partial(final_kernel, step_size),
            out_shape=jax.ShapeDtypeStruct((num_ens, num_part, loc_feat), f32),
            in_specs=[vmem] * 4,
            out_specs=hbm,
            scratch_shapes=[pltpu.VMEM((tiles, num_part, TILE), f32), dma((num_ens - 1 + tiles,))],
            compiler_params=pltpu.CompilerParams(vmem_limit_bytes=FINAL_LIMIT),
            name="final_update",
        )(theta, kern, sums, yn)

    return jax.shard_map(local_steps, mesh=mesh, in_specs=(data_spec, mean_spec, prec_spec, factor_spec),
                         out_specs=data_spec, check_vma=False)
```
